512 devices in a mesh: energy: 16 (over z, core), rows: 32 (over y, x).
Axes of the slice: x: 4, y: 8, z: 8, core: 2. Of those that a mesh axis runs over, the one named last changes fastest.
Arguments:
- coupling: bfloat16 [2, 512, 512], replicated, may hold values from -4.1875 to 4.1875
- inverses: bfloat16 [512, 4, 2, 256, 256], P(('energy', 'rows')), may hold values from -0.0078125 to 0.0078125
- contact_row: int32 [48], replicated, may hold values from 0 to 31, as said below
- assignment: int32 [128], P('energy'), may hold values from 0 to 127, as said below
- states: bfloat16 [48, 2, 16, 512], replicated, may hold values from -0.119628906 to 0.119628906
- weights: float32 [128], P('energy'), may hold values from 0.03 to 0.3
Outputs:
- injection: float32 [128, 32, 2, 16, 512], P('energy', 'rows')
- integrated: float32 [32, 2, 16, 512], P('rows')
- far_forward: bfloat16 [512, 2, 256, 256], P(('energy', 'rows'))
- far_backward: bfloat16 [512, 2, 256, 256], P(('energy', 'rows'))
The draws below stay inside these ranges and needn't reach their ends.
Inputs may be any that keep to these rules, and one draw needn't show every extreme that they name: `contact_row`: every device block row has one contact or more. `assignment`: each aligned block of 8 entries, b * 8 to b * 8 + 7, holds each of those same numbers once.
All inputs are finite; a program needn't handle non-finite values.
Results may differ from the reference program's by a relative error of at most 0.024.
Values may be sent and summed in bfloat16 or wider, within the bound.
No kernel may reach another device: no remote copies, remote signals or barrier semaphores. Data moves between devices by JAX's collectives and lax.ppermute only.
A program may use at most 64 MiB of HBM per device.

```python
import math
import jax
import jax.numpy as jnp
from jax import lax

ORBITALS = 512
ITERS = 4
STATES = 16
HALF = 256
GROUPS = 8
ENERGIES = 128
QUARTERS = 512
BLOCK_ROWS = 32
CONTACTS = 48


def draw_contact_row(key, part):
    first_key, second_key, third_key = jax.random.split(jax.random.fold_in(key, 11), 3)
    covering = jax.random.permutation(first_key, BLOCK_ROWS).astype(jnp.int32)
    extra_rows = jax.random.randint(second_key, (CONTACTS - BLOCK_ROWS,), 0, BLOCK_ROWS).astype(jnp.int32)
    joined = jnp.concatenate([covering, extra_rows])
    shuffle = jax.random.permutation(third_key, CONTACTS)
    return jnp.take(joined, shuffle).astype(jnp.int32)


def block_permutation(block_key):
    return jax.random.permutation(block_key, GROUPS).astype(jnp.int32)


def draw_assignment(key, part):
    block_keys = jax.random.split(jax.random.fold_in(key, 23), ENERGIES // GROUPS)
    blocks = jax.vmap(block_permutation)(block_keys)
    offsets = (jnp.arange(ENERGIES // GROUPS, dtype=jnp.int32) * GROUPS)[:, None]
    return (blocks + offsets).reshape(ENERGIES).astype(jnp.int32)


def block_scale(stream_key, shape, shards, low, top_value):
    level, own = 1.0, jax.random.fold_in(stream_key, 6)
    for dim, parts in shards:
        draws = jnp.exp(jax.random.uniform(jax.random.fold_in(own, dim), (parts,), jnp.float32, low / len(shards), top_value / len(shards)))
        level = level * jnp.repeat(draws, shape[dim] // parts).reshape([-1 if axis == dim else 1 for axis in range(len(shape))])
    return level


def normal_values(stream_key, shape, width, most, shards=(), kind=jnp.bfloat16):
    array = jax.random.normal(stream_key, shape, jnp.float32) * width
    if len(shards) > 0:
        array = block_scale(stream_key, shape, shards, -0.22, 0.18) * array
    return jnp.clip(array, min=-most, max=most).astype(kind)


def setup_inputs(seed: int = 0) -> dict:
    key_list = jax.random.split(jax.random.key(seed), 7)
    coupling = normal_values(key_list[0], (2, ORBITALS, ORBITALS), 0.7, 4.1875)
    inverses = normal_values(key_list[1], (QUARTERS, ITERS, 2, HALF, HALF), (2 * ORBITALS * ORBITALS) ** -0.5, 0.0078125, ((0, 512),))
    contact_row = draw_contact_row(jax.random.fold_in(key_list[6], 71), 0)
    assignment = draw_assignment(jax.random.fold_in(key_list[6], 71), 0)
    states = normal_values(key_list[4], (CONTACTS, 2, STATES, ORBITALS), 0.02, 0.119628906)
    weights = jnp.clip(jnp.exp(math.log(0.3) - 2.3025852 * jax.random.uniform(key_list[5], (ENERGIES,), jnp.float32) ** block_scale(key_list[5], (ENERGIES,), ((0, 16),), -0.2, 0.2)), 0.03, 0.3)
    return {"coupling": coupling, "inverses": inverses, "contact_row": contact_row, "assignment": assignment, "states": states, "weights": weights}


def complex_dot(left_matrix, right_matrix):
    def single(leading, trailing):
        return jnp.dot(leading.astype(jnp.float32), trailing.astype(jnp.float32), preferred_element_type=jnp.float32)
    real_part = single(left_matrix[0], right_matrix[0]) - single(left_matrix[1], right_matrix[1])
    imag_part = single(left_matrix[0], right_matrix[1]) + single(left_matrix[1], right_matrix[0])
    return jnp.stack([real_part, imag_part])


def reference(coupling, inverses, contact_row, assignment, states, weights):
    half_order = ORBITALS // 2

    def assemble(blocks):
        shaped = blocks.reshape(2, 2, ITERS, 2, half_order, half_order)
        return shaped.transpose(2, 3, 0, 4, 1, 5).reshape(ITERS, 2, ORBITALS, ORBITALS)

    def split_blocks(matrix):
        shaped = matrix.reshape(2, 2, half_order, 2, half_order)
        return shaped.transpose(1, 3, 0, 2, 4).reshape(4, 2, half_order, half_order)

    forward_start = coupling
    backward_start = jnp.stack([coupling[0].T, -coupling[1].T])
    row_ids = jnp.arange(BLOCK_ROWS, dtype=jnp.int32)
    selector = (contact_row[None, :] == row_ids[:, None]).astype(jnp.float32)
    drive = jnp.dot(selector, states.reshape(CONTACTS, -1).astype(jnp.float32), preferred_element_type=jnp.float32)
    drive = drive.astype(jnp.bfloat16).reshape(BLOCK_ROWS, 2, STATES, ORBITALS)
    drive_real = drive[:, 0].reshape(BLOCK_ROWS * STATES, ORBITALS).astype(jnp.float32)
    drive_imag = drive[:, 1].reshape(BLOCK_ROWS * STATES, ORBITALS).astype(jnp.float32)

    def per_slot(blocks):
        inverse_all = assemble(blocks)
        forward = forward_start
        backward = backward_start
        surface_sum = jnp.zeros((2, ORBITALS, ORBITALS), jnp.float32)
        for iteration in range(ITERS):
            forward_green = complex_dot(forward, inverse_all[iteration]).astype(jnp.bfloat16)
            backward_green = complex_dot(backward, inverse_all[iteration]).astype(jnp.bfloat16)
            surface_sum = surface_sum + complex_dot(forward_green, backward)
            forward_next = complex_dot(forward_green, forward).astype(jnp.bfloat16)
            backward = complex_dot(backward_green, backward).astype(jnp.bfloat16)
            forward = forward_next
        self_energy = surface_sum.astype(jnp.bfloat16).astype(jnp.float32)
        energy_real = self_energy[0].T
        energy_imag = self_energy[1].T
        real_part = jnp.dot(drive_real, energy_real, preferred_element_type=jnp.float32) - jnp.dot(drive_imag, energy_imag, preferred_element_type=jnp.float32)
        imag_part = jnp.dot(drive_imag, energy_real, preferred_element_type=jnp.float32) + jnp.dot(drive_real, energy_imag, preferred_element_type=jnp.float32)
        injected = jnp.stack([real_part.reshape(BLOCK_ROWS, STATES, ORBITALS), imag_part.reshape(BLOCK_ROWS, STATES, ORBITALS)], axis=1)
        return injected, split_blocks(forward), split_blocks(backward)

    slot_blocks = inverses.reshape(ENERGIES, 4, ITERS, 2, half_order, half_order)
    slot_injection, far_fwd, far_bwd = lax.map(per_slot, slot_blocks)
    injection = jnp.zeros_like(slot_injection).at[assignment].set(slot_injection)
    integrated = jnp.tensordot(weights, injection, axes=1, precision=lax.Precision.HIGHEST)
    far_forward = far_fwd.reshape(QUARTERS, 2, half_order, half_order)
    far_backward = far_bwd.reshape(QUARTERS, 2, half_order, half_order)
    return injection, integrated, far_forward, far_backward
```

```python
import jax
import jax.numpy as jnp
from jax import lax
from jax.experimental import pallas as pl
from jax.experimental.pallas import tpu as pltpu
from jax.sharding import PartitionSpec as P


ITERS = 4
CHUNK = 2
FLIPS = (1, 3, 2)
VMEM_WHOLE = pl.BlockSpec(memory_space=pltpu.VMEM)
SMEM_WHOLE = pl.BlockSpec(memory_space=pltpu.SMEM)
HBM_WHOLE = pl.BlockSpec(memory_space=pltpu.HBM)
MIB = 1 << 20


def dot(left, right):
    return jnp.dot(left, right, preferred_element_type=jnp.float32)


def row_bit():
    return lax.rem(lax.div(lax.axis_index("rows"), 2), 2)


def core_bit():
    return lax.rem(lax.axis_index("energy"), 2)


def embed(ref, rows, columns, real, imag):
    high = ref.shape[0] // 2
    wide = ref.shape[1] // 2
    (r0, r1), (c0, c1) = rows, columns
    ref[r0:r1, c0:c1] = real
    ref[high + r0 : high + r1, c0:c1] = imag
    ref[r0:r1, wide + c0 : wide + c1] = -imag
    ref[high + r0 : high + r1, wide + c0 : wide + c1] = real


def prepare(row_ref, coupling_ref, states_ref, forward_ref, backward_ref, drive_ref, sums):
    order = coupling_ref.shape[-1]
    whole = ((0, order), (0, order))
    real, imag = coupling_ref[0], coupling_ref[1]
    embed(forward_ref, *whole, real, imag)
    embed(backward_ref, *whole, real.T, -imag.T)
    sums[...] = jnp.zeros_like(sums)
    for contact in range(states_ref.shape[0]):
        row = row_ref[contact]
        sums[row] = sums[row] + states_ref[contact].astype(jnp.float32)
    drive = sums[...].astype(jnp.bfloat16)
    block_rows, _, count, _ = drive.shape
    count = block_rows * count
    embed(
        drive_ref,
        (0, count),
        (0, order),
        drive[:, 0].reshape(count, order),
        drive[:, 1].reshape(count, order),
    )


def assemble(step, fetched, green):
    row, column = row_bit(), core_bit()
    own_ref, side_ref, cross_ref, down_ref = fetched
    half = own_ref.shape[-1]
    for blocks, a, b in (
        (own_ref, row, column),
        (side_ref, row, 1 - column),
        (cross_ref, 1 - row, 1 - column),
        (down_ref, 1 - row, column),
    ):
        for part in range(2):
            start = pl.multiple_of(part * 2 * half + a * half, half)
            green[b, pl.ds(start, half), :] = blocks[step, part]


def own_rows(matrix, part):
    half = matrix.shape[0] // 4
    start = pl.multiple_of(part * 2 * half + row_bit() * half, half)
    return matrix[pl.ds(start, half), :]


def step_products(source, target, green, products, surface_from, surface):
    order = source[0].shape[0] // 2
    half = order // 2
    for coupling, product in zip(source, products):
        for b in range(2):
            value = dot(coupling[...], green[b]).astype(jnp.bfloat16)
            embed(product, (0, order), (b * half, (b + 1) * half), value[:order], value[order:])
    for part in range(2):
        term = dot(own_rows(products[0], part), source[1][:, :order])
        surface[part] = term if surface_from is None else surface_from[part] + term
    for product, coupling, following in zip(products, source, target):
        for b in range(2):
            columns = (b * half, (b + 1) * half)
            value = dot(product[...], coupling[:, columns[0] : columns[1]]).astype(jnp.bfloat16)
            embed(following, (0, order), columns, value[:order], value[order:])


def first_steps(
    forward_in, backward_in, own_ref, side_ref, cross_ref, down_ref,
    forward, backward, surface, green, forward_green, backward_green,
):
    source, target = (forward_in, backward_in), (forward, backward)
    surface_from = None
    for step in range(CHUNK):
        assemble(step, (own_ref, side_ref, cross_ref, down_ref), green)
        step_products(source, target, green, (forward_green, backward_green), surface_from, surface)
        source, surface_from = target, surface


def last_steps(
    forward_in, backward_in, surface_in, drive_ref, own_ref, side_ref, cross_ref, down_ref,
    forward_out, backward_out, green_out, forward_rows_out, injected,
    forward, backward, green, forward_rows, surface, forward_green, backward_green, copy_sems,
):
    fetched = (own_ref, side_ref, cross_ref, down_ref)
    leaving = (forward, backward, green, forward_rows)
    outs = (forward_out, backward_out, green_out, forward_rows_out)
    copies = [
        pltpu.make_async_copy(kept, out, copy_sems.at[i])
        for i, (kept, out) in enumerate(zip(leaving, outs))
    ]
    source, target = (forward_in, backward_in), (forward, backward)
    surface_from = surface_in
    for step in range(CHUNK - 1):
        assemble(step, fetched, green)
        step_products(source, target, green, (forward_green, backward_green), surface_from, surface)
        source, surface_from = target, surface
    copies[0].start()
    copies[1].start()
    assemble(CHUNK - 1, fetched, green)
    copies[2].start()
    order = forward.shape[0] // 2
    half = order // 2
    for b in range(2):
        columns = (b * half, (b + 1) * half)
        real = dot(own_rows(forward, 0), green[b]).astype(jnp.bfloat16)
        imag = dot(own_rows(forward, 1), green[b]).astype(jnp.bfloat16)
        embed(forward_rows, (0, half), columns, real, imag)
    copies[3].start()
    energy = []
    for part in range(2):
        rows = forward_rows[part * half : (part + 1) * half, :]
        energy.append((surface[part] + dot(rows, backward[:, :order])).astype(jnp.bfloat16))
    value = lax.dot_general(
        drive_ref[...],
        jnp.concatenate(energy, axis=1),
        (((1,), (1,)), ((), ())),
        preferred_element_type=jnp.float32,
    ).astype(jnp.bfloat16)
    block_rows, _, count, _ = injected.shape
    rows = block_rows * count
    for part in range(2):
        injected[:, part] = value[part * rows : (part + 1) * rows].reshape(block_rows, count, half)
    for copy in copies:
        copy.wait()


def far_blocks(forward, backward, green, forward_rows, kept_ref, given_ref, backward_rows):
    order = forward.shape[0] // 2
    half = order // 2
    core = core_bit()
    for b in range(2):
        columns = (b * half, (b + 1) * half)
        real = dot(own_rows(backward, 0), green[b]).astype(jnp.bfloat16)
        imag = dot(own_rows(backward, 1), green[b]).astype(jnp.bfloat16)
        embed(backward_rows, (0, half), columns, real, imag)
    for which, rows, coupling in ((0, forward_rows, forward), (1, backward_rows, backward)):
        for b in range(2):
            for part in range(2):
                value = dot(
                    rows[part * half : (part + 1) * half, :],
                    coupling[:, b * half : (b + 1) * half],
                ).astype(jnp.bfloat16)

                @pl.when(core == b)
                def _():
                    kept_ref[which, part] = value

                @pl.when(core != b)
                def _():
                    given_ref[which, part] = value


def spread(assignment_ref, weight_ref, received_ref, injection_ref, weighted_ref):
    groups = injection_ref.shape[0]
    half = received_ref.shape[-1]
    column = core_bit()
    for part in range(2):
        for a in range(2):
            total = jnp.zeros(injection_ref.shape[2:3] + (half,), jnp.float32)
            for slot in range(groups):
                e = lax.rem(assignment_ref[slot], groups)
                value = received_ref[slot, a, column, part].astype(jnp.float32)
                injection_ref[e, part, :, a * half : (a + 1) * half] = value
                total = total + weight_ref[e] * value
            total = total.astype(weighted_ref.dtype)
            for copy in range(weighted_ref.shape[0]):
                weighted_ref[copy, part, :, a * half : (a + 1) * half] = total


def call(body, outs, scratch, scalars=0, vmem=32, far_outs=0):
    def run(*operands):
        specs = [SMEM_WHOLE] * scalars + [VMEM_WHOLE] * (len(operands) - scalars)
        return pl.pallas_call(
            body,
            out_shape=outs,
            in_specs=specs,
            out_specs=tuple(HBM_WHOLE if i < far_outs else VMEM_WHOLE for i in range(len(outs))),
            scratch_shapes=scratch,
            compiler_params=pltpu.CompilerParams(vmem_limit_bytes=vmem * MIB),
        )(*operands)

    return run


def local(energies_axis, rows_axis, coupling, inverses, contact_row, assignment, states, weights):
    half = inverses.shape[-1]
    order = 2 * half
    slots = rows_axis // 4
    bf16, f32 = jnp.bfloat16, jnp.float32
    both = ("energy", "rows")

    def routes(flip, to_worker):
        pairs = []
        for energy in range(energies_axis):
            for slot in range(slots):
                for x in range(4):
                    if (x % 2 == energy % 2) == to_worker:
                        base = energy * rows_axis + slot * 4
                        pairs.append((base + (x ^ flip), base + x))
        return pairs

    chunks = [inverses[0, CHUNK * c : CHUNK * (c + 1)] for c in range(ITERS // CHUNK)]
    fetched = []
    for c, chunk in enumerate(chunks):
        fetched.append([])
        for flip in FLIPS:
            fetched[c].append(lax.ppermute(chunk, both, routes(flip, True)))

    square = jax.ShapeDtypeStruct((2 * order, 2 * order), bf16)
    count = states.shape[2]
    block_rows = rows_axis
    forward, backward, drive = call(
        prepare,
        (square, square, jax.ShapeDtypeStruct((2 * block_rows * count, 2 * order), bf16)),
        [pltpu.VMEM((block_rows, 2, count, order), f32)],
        scalars=1,
    )(contact_row, coupling, states)

    square_scratch = pltpu.VMEM((2 * order, 2 * order), bf16)
    green_shape = (2, 2 * order, half)
    surface_shape = (2, half, order)
    forward, backward, surface = call(
        first_steps,
        (square, square, jax.ShapeDtypeStruct(surface_shape, f32)),
        [pltpu.VMEM(green_shape, bf16), square_scratch, square_scratch],
    )(forward, backward, chunks[0], *fetched[0])
    forward, backward, green, forward_rows, injected = call(
        last_steps,
        (
            pltpu.HBM((2 * order, 2 * order), bf16),
            pltpu.HBM((2 * order, 2 * order), bf16),
            pltpu.HBM(green_shape, bf16),
            pltpu.HBM((order, 2 * order), bf16),
            jax.ShapeDtypeStruct((block_rows, 2, count, half), bf16),
        ),
        [
            square_scratch,
            square_scratch,
            pltpu.VMEM(green_shape, bf16),
            pltpu.VMEM((order, 2 * order), bf16),
            pltpu.VMEM(surface_shape, f32),
            square_scratch,
            square_scratch,
            pltpu.SemaphoreType.DMA((4,)),
        ],
        far_outs=4,
    )(forward, backward, surface, drive, chunks[1], *fetched[1])

    received = lax.all_to_all(injected, "rows", split_axis=0, concat_axis=0, tiled=True)

    far_shape = jax.ShapeDtypeStruct((2, 2, half, half), bf16)
    kept, given = call(
        far_blocks, (far_shape, far_shape), [pltpu.VMEM((order, 2 * order), bf16)]
    )(forward, backward, green, forward_rows)
    given = lax.ppermute(given, both, routes(1, False))
    worker = lax.axis_index("rows") % 2 == core_bit()
    far_out = jnp.where(worker, kept, given)

    groups = assignment.shape[0]
    chips = energies_axis // 2
    injection, weighted = call(
        spread,
        (
            jax.ShapeDtypeStruct((groups, 2, count, order), f32),
            jax.ShapeDtypeStruct((chips, 2, count, order), bf16),
        ),
        [],
        scalars=2,
    )(assignment, weights, received.reshape(slots, 2, 2, 2, count, half))
    alike = [[2 * chip + core for chip in range(chips)] for core in range(2)]
    gathered = lax.all_to_all(
        weighted, "energy", split_axis=0, concat_axis=0, axis_index_groups=alike, tiled=True
    )
    part_sum = jnp.sum(gathered.astype(f32), axis=0)
    other_sum = lax.ppermute(
        part_sum.astype(bf16), "energy", [(i, i ^ 1) for i in range(energies_axis)]
    )
    integrated = part_sum + other_sum.astype(f32)
    return injection[:, None], integrated[None], far_out[0][None], far_out[1][None]


def solution(mesh):
    def whole(*operands):
        return local(mesh.shape["energy"], mesh.shape["rows"], *operands)

    placed = (
        P(),
        P(("energy", "rows"), None, None, None, None),
        P(),
        P("energy"),
        P(),
        P("energy"),
    )
    return jax.shard_map(
        whole,
        mesh=mesh,
        in_specs=placed,
        out_specs=(
            P("energy", "rows", None, None, None),
            P("rows", None, None, None),
            P(("energy", "rows"), None, None, None),
            P(("energy", "rows"), None, None, None),
        ),
        check_vma=False,
    )
```

```python
import functools

import jax
import jax.numpy as jnp
from jax import lax
from jax.experimental import pallas as pl
from jax.experimental.pallas import tpu as pltpu
from jax.sharding import PartitionSpec as P


ITERS = 4
CHUNK = 2
FLIPS = (1, 3, 2)
VMEM_WHOLE = pl.BlockSpec(memory_space=pltpu.VMEM)
SMEM_WHOLE = pl.BlockSpec(memory_space=pltpu.SMEM)
HBM_WHOLE = pl.BlockSpec(memory_space=pltpu.HBM)
MIB = 1 << 20


def dot(left, right):
    return jnp.dot(left, right, preferred_element_type=jnp.float32)


def row_bit():
    return lax.rem(lax.div(lax.axis_index("rows"), 2), 2)


def core_bit():
    return lax.rem(lax.axis_index("energy"), 2)


def place(ref, column_half, value):
    half = value.shape[1]
    start = column_half * 2 * half
    ref[:, start : start + half] = value
    for row in range(0, value.shape[0], 2 * half):
        ref[row : row + half, start + half : start + 2 * half] = -value[row + half : row + 2 * half]
        ref[row + half : row + 2 * half, start + half : start + 2 * half] = value[row : row + half]


def column_of(matrix, column_half):
    half = matrix.shape[1] // 4
    return matrix[:, column_half * 2 * half : column_half * 2 * half + half]


def prepare(row_ref, coupling_ref, states_ref, forward_ref, backward_ref, drive_ref, sums):
    order = coupling_ref.shape[-1]
    half = order // 2
    sums[...] = jnp.zeros_like(sums)

    @pl.loop(0, states_ref.shape[0])
    def _(contact):
        row = row_ref[contact]
        sums[row] = sums[row] + states_ref[contact].astype(jnp.float32)

    block_rows, _, count, _ = sums.shape
    count = block_rows * count

    def arrange(first):
        def block(part, i, j):
            rows, columns = ((first ^ k) * half for k in (i, j))
            return coupling_ref[part, rows : rows + half, columns : columns + half]

        for j in range(2):
            ahead, back = [], []
            for i in range(2):
                ahead += [block(0, i, j), block(1, i, j)]
                back += [block(0, j, i).T, -block(1, j, i).T]
            place(forward_ref, j, jnp.concatenate(ahead, axis=0))
            place(backward_ref, j, jnp.concatenate(back, axis=0))
        for h in range(2):
            left = h * half
            right = order + left
            start = (first ^ h) * half
            real, imag = (
                sums[:, part, :, start : start + half].astype(jnp.bfloat16).reshape(count, half)
                for part in range(2)
            )
            drive_ref[:count, left : left + half] = real
            drive_ref[count:, left : left + half] = imag
            drive_ref[:count, right : right + half] = -imag
            drive_ref[count:, right : right + half] = real

    for first in range(2):
        pl.when(row_bit() == first)(functools.partial(arrange, first))


def assemble(step, fetched, green):
    own_ref, side_ref, cross_ref, down_ref = fetched
    half = own_ref.shape[-1]

    def fill(mine):
        for blocks, row, column in (
            (own_ref, 0, mine),
            (side_ref, 0, 1 - mine),
            (cross_ref, 1, 1 - mine),
            (down_ref, 1, mine),
        ):
            for part in range(2):
                start = (2 * row + part) * half
                green[column, start : start + half, :] = blocks[step, part]

    for mine in range(2):
        pl.when(lax.rem(row_bit() + core_bit(), 2) == mine)(functools.partial(fill, mine))


def step_products(source, target, green, products, surface_from, surface):
    order = source[0].shape[0] // 2
    half = order // 2
    for coupling, product in zip(source, products):
        for h in range(2):
            place(product, h, dot(coupling[...], green[h]).astype(jnp.bfloat16))
    for h in range(2):
        term = dot(products[0][:order, :], column_of(source[1], h))
        columns = slice(h * half, (h + 1) * half)
        surface[:, columns] = term if surface_from is None else surface_from[:, columns] + term
    for product, coupling, following in zip(products, source, target):
        for h in range(2):
            place(following, h, dot(product[...], column_of(coupling, h)).astype(jnp.bfloat16))


def first_steps(
    forward_in, backward_in, own_ref, side_ref, cross_ref, down_ref,
    forward, backward, surface, green, forward_green, backward_green,
):
    source, target = (forward_in, backward_in), (forward, backward)
    surface_from = None
    for step in range(CHUNK):
        assemble(step, (own_ref, side_ref, cross_ref, down_ref), green)
        step_products(source, target, green, (forward_green, backward_green), surface_from, surface)
        source, surface_from = target, surface


def last_steps(
    forward_in, backward_in, surface_in, drive_ref, own_ref, side_ref, cross_ref, down_ref,
    forward_out, backward_out, green_out, forward_rows_out, injected,
    forward, backward, green, forward_rows, surface, forward_green, backward_green, copy_sems,
):
    fetched = (own_ref, side_ref, cross_ref, down_ref)
    leaving = (forward, backward, green, forward_rows)
    outs = (forward_out, backward_out, green_out, forward_rows_out)
    copies = [
        pltpu.make_async_copy(kept, out, copy_sems.at[i])
        for i, (kept, out) in enumerate(zip(leaving, outs))
    ]
    source, target = (forward_in, backward_in), (forward, backward)
    surface_from = surface_in
    for step in range(CHUNK - 1):
        assemble(step, fetched, green)
        step_products(source, target, green, (forward_green, backward_green), surface_from, surface)
        source, surface_from = target, surface
    copies[0].start()
    copies[1].start()
    assemble(CHUNK - 1, fetched, green)
    copies[2].start()
    order = forward.shape[0] // 2
    half = order // 2
    for h in range(2):
        place(forward_rows, h, dot(forward[:order, :], green[h]).astype(jnp.bfloat16))
    copies[3].start()
    energy = []
    for h in range(2):
        term = dot(forward_rows[...], column_of(backward, h))
        energy.append((surface[:, h * half : (h + 1) * half] + term).astype(jnp.bfloat16))
    value = lax.dot_general(
        drive_ref[...],
        jnp.concatenate([e[part * half : (part + 1) * half] for part in range(2) for e in energy], axis=1),
        (((1,), (1,)), ((), ())),
        preferred_element_type=jnp.float32,
    ).astype(jnp.bfloat16)
    block_rows, _, count, _ = injected.shape
    rows = block_rows * count
    for part in range(2):
        injected[:, part] = value[part * rows : (part + 1) * rows].reshape(block_rows, count, half)
    for copy in copies:
        copy.wait()


def far_blocks(
    forward_in, backward_in, green_in, forward_rows_in, kept_ref, given_ref,
    forward, backward, green, forward_rows, backward_rows, copy_sems,
):
    arriving = (backward_in, green_in, forward_rows_in, forward_in)
    held = (backward, green, forward_rows, forward)
    copies = [
        pltpu.make_async_copy(source, kept, copy_sems.at[i])
        for i, (source, kept) in enumerate(zip(arriving, held))
    ]
    for copy in copies:
        copy.start()
    order = forward.shape[0] // 2
    half = order // 2
    mine = lax.rem(row_bit() + core_bit(), 2)
    copies[0].wait()
    copies[1].wait()
    for h in range(2):
        place(backward_rows, h, dot(backward[:order, :], green[h]).astype(jnp.bfloat16))
    copies[2].wait()
    copies[3].wait()
    for which, rows, coupling in ((0, forward_rows, forward), (1, backward_rows, backward)):
        for h in range(2):
            value = dot(rows[...], column_of(coupling, h)).astype(jnp.bfloat16)

            @pl.when(mine == h)
            def _():
                kept_ref[which, 0] = value[:half]
                kept_ref[which, 1] = value[half:]

            @pl.when(mine != h)
            def _():
                given_ref[which, 0] = value[:half]
                given_ref[which, 1] = value[half:]


def choose(kept_ref, given_ref, forward_ref, backward_ref):
    worker = lax.rem(lax.axis_index("rows"), 2) == core_bit()
    for which, far_ref in enumerate((forward_ref, backward_ref)):
        far_ref[0] = jnp.where(worker, kept_ref[which], given_ref[which])


def spread(assignment_ref, weight_ref, received_ref, injection_ref, weighted_ref):
    groups = injection_ref.shape[0]
    half = received_ref.shape[-1]
    column = core_bit()
    for part in range(2):
        for a in range(2):
            total = jnp.zeros(injection_ref.shape[2:3] + (half,), jnp.float32)
            for slot in range(groups):
                e = lax.rem(assignment_ref[slot], groups)
                value = received_ref[slot, a, column, part].astype(jnp.float32)
                injection_ref[e, part, :, a * half : (a + 1) * half] = value
                total = total + weight_ref[e] * value
            total = total.astype(weighted_ref.dtype)
            for copy in range(weighted_ref.shape[0]):
                weighted_ref[copy, part, :, a * half : (a + 1) * half] = total


def in_hbm(*arrays):
    return [pltpu.with_memory_space_constraint(array, pltpu.HBM) for array in arrays]


def call(body, outs, scratch, scalars=0, vmem=32, far_outs=0, far_ins=0):
    def run(*operands):
        specs = [SMEM_WHOLE] * scalars + [VMEM_WHOLE] * (len(operands) - scalars)
        specs[:far_ins] = [HBM_WHOLE] * far_ins
        return pl.pallas_call(
            body,
            out_shape=outs,
            in_specs=specs,
            out_specs=tuple(HBM_WHOLE if i < far_outs else VMEM_WHOLE for i in range(len(outs))),
            scratch_shapes=scratch,
            compiler_params=pltpu.CompilerParams(vmem_limit_bytes=vmem * MIB),
        )(*operands)

    return run


def local(energies_axis, rows_axis, coupling, inverses, contact_row, assignment, states, weights):
    half = inverses.shape[-1]
    order = 2 * half
    slots = rows_axis // 4
    bf16, f32 = jnp.bfloat16, jnp.float32
    both = ("energy", "rows")

    def routes(flip, to_worker):
        pairs = []
        for energy in range(energies_axis):
            for slot in range(slots):
                for x in range(4):
                    if (x % 2 == energy % 2) == to_worker:
                        base = energy * rows_axis + slot * 4
                        pairs.append((base + (x ^ flip), base + x))
        return pairs

    chunks = [inverses[0, CHUNK * c : CHUNK * (c + 1)] for c in range(ITERS // CHUNK)]
    fetched = []
    for c, chunk in enumerate(chunks):
        fetched.append([])
        for flip in FLIPS:
            fetched[c].append(lax.ppermute(chunk, both, routes(flip, True)))

    square = jax.ShapeDtypeStruct((2 * order, 2 * order), bf16)
    count = states.shape[2]
    block_rows = rows_axis
    forward, backward, drive = call(
        prepare,
        (square, square, jax.ShapeDtypeStruct((2 * block_rows * count, 2 * order), bf16)),
        [pltpu.VMEM((block_rows, 2, count, order), f32)],
        scalars=1,
    )(contact_row, coupling, states)

    square_scratch = pltpu.VMEM((2 * order, 2 * order), bf16)
    green_shape = (2, 2 * order, half)
    surface_shape = (order, order)
    rows_scratch = pltpu.VMEM((order, 2 * order), bf16)
    forward, backward, surface = call(
        first_steps,
        (square, square, jax.ShapeDtypeStruct(surface_shape, f32)),
        [pltpu.VMEM(green_shape, bf16), square_scratch, square_scratch],
    )(forward, backward, chunks[0], *fetched[0])
    forward, backward, green, forward_rows, injected = call(
        last_steps,
        (
            pltpu.HBM((2 * order, 2 * order), bf16),
            pltpu.HBM((2 * order, 2 * order), bf16),
            pltpu.HBM(green_shape, bf16),
            pltpu.HBM((order, 2 * order), bf16),
            jax.ShapeDtypeStruct((block_rows, 2, count, half), bf16),
        ),
        [
            square_scratch,
            square_scratch,
            pltpu.VMEM(green_shape, bf16),
            rows_scratch,
            pltpu.VMEM(surface_shape, f32),
            square_scratch,
            square_scratch,
            pltpu.SemaphoreType.DMA((4,)),
        ],
        far_outs=4,
    )(forward, backward, surface, drive, chunks[1], *fetched[1])

    received = lax.all_to_all(injected, "rows", split_axis=0, concat_axis=0, tiled=True)

    far_shape = jax.ShapeDtypeStruct((2, 2, half, half), bf16)
    kept, given = call(
        far_blocks,
        (far_shape, far_shape),
        [
            square_scratch,
            square_scratch,
            pltpu.VMEM(green_shape, bf16),
            rows_scratch,
            rows_scratch,
            pltpu.SemaphoreType.DMA((4,)),
        ],
        far_ins=4,
    )(*in_hbm(forward, backward, green, forward_rows))
    given = lax.ppermute(given, both, routes(1, False))
    block_shape = jax.ShapeDtypeStruct((1, 2, half, half), bf16)
    far_forward, far_backward = call(choose, (block_shape, block_shape), [])(kept, given)

    groups = assignment.shape[0]
    chips = energies_axis // 2
    injection, weighted = call(
        spread,
        (
            jax.ShapeDtypeStruct((groups, 2, count, order), f32),
            jax.ShapeDtypeStruct((chips, 2, count, order), bf16),
        ),
        [],
        scalars=2,
    )(assignment, weights, received.reshape(slots, 2, 2, 2, count, half))
    alike = [[2 * chip + core for chip in range(chips)] for core in range(2)]
    gathered = lax.all_to_all(
        weighted, "energy", split_axis=0, concat_axis=0, axis_index_groups=alike, tiled=True
    )
    part_sum = jnp.sum(gathered.astype(f32), axis=0)
    other_sum = lax.ppermute(
        part_sum.astype(bf16), "energy", [(i, i ^ 1) for i in range(energies_axis)]
    )
    integrated = part_sum + other_sum.astype(f32)
    return injection[:, None], integrated[None], far_forward, far_backward


def solution(mesh):
    def whole(*operands):
        return local(mesh.shape["energy"], mesh.shape["rows"], *operands)

    placed = (
        P(),
        P(("energy", "rows"), None, None, None, None),
        P(),
        P("energy"),
        P(),
        P("energy"),
    )
    return jax.shard_map(
        whole,
        mesh=mesh,
        in_specs=placed,
        out_specs=(
            P("energy", "rows", None, None, None),
            P("rows", None, None, None),
            P(("energy", "rows"), None, None, None),
            P(("energy", "rows"), None, None, None),
        ),
        check_vma=False,
    )
```

```python
import functools

import jax
import jax.numpy as jnp
from jax import lax
from jax.experimental import pallas as pl
from jax.experimental.pallas import tpu as pltpu
from jax.sharding import PartitionSpec as P


ITERS = 4
CHUNK = 2
FLIPS = (1, 3, 2)
VMEM_WHOLE = pl.BlockSpec(memory_space=pltpu.VMEM)
SMEM_WHOLE = pl.BlockSpec(memory_space=pltpu.SMEM)
HBM_WHOLE = pl.BlockSpec(memory_space=pltpu.HBM)
MIB = 1 << 20


def dot(left, right):
    return jnp.dot(left, right, preferred_element_type=jnp.float32)


def row_bit():
    return lax.rem(lax.div(lax.axis_index("rows"), 2), 2)


def core_bit():
    return lax.rem(lax.axis_index("energy"), 2)


def place(ref, column_half, value):
    half = value.shape[1]
    start = column_half * 2 * half
    ref[:, start : start + half] = value
    for row in range(0, value.shape[0], 2 * half):
        ref[row : row + half, start + half : start + 2 * half] = -value[row + half : row + 2 * half]
        ref[row + half : row + 2 * half, start + half : start + 2 * half] = value[row : row + half]


def column_of(matrix, column_half):
    half = matrix.shape[1] // 4
    return matrix[:, column_half * 2 * half : column_half * 2 * half + half]


def prepare(row_ref, coupling_ref, states_ref, forward_ref, backward_ref, drive_ref, sums):
    order = coupling_ref.shape[-1]
    half = order // 2
    sums[...] = jnp.zeros_like(sums)

    @pl.loop(0, states_ref.shape[0])
    def _(contact):
        row = row_ref[contact]
        sums[row] = sums[row] + states_ref[contact].astype(jnp.float32)

    block_rows, _, count, _ = sums.shape
    count = block_rows * count

    def arrange(first):
        def block(part, i, j):
            rows, columns = ((first ^ k) * half for k in (i, j))
            return coupling_ref[part, rows : rows + half, columns : columns + half]

        for j in range(2):
            ahead, back = [], []
            for i in range(2):
                ahead += [block(0, i, j), block(1, i, j)]
                back += [block(0, j, i).T, -block(1, j, i).T]
            place(forward_ref, j, jnp.concatenate(ahead, axis=0))
            place(backward_ref, j, jnp.concatenate(back, axis=0))
        for h in range(2):
            left = h * half
            right = order + left
            start = (first ^ h) * half
            real, imag = (
                sums[:, part, :, start : start + half].astype(jnp.bfloat16).reshape(count, half)
                for part in range(2)
            )
            drive_ref[:count, left : left + half] = real
            drive_ref[count:, left : left + half] = imag
            drive_ref[:count, right : right + half] = -imag
            drive_ref[count:, right : right + half] = real

    for first in range(2):
        pl.when(row_bit() == first)(functools.partial(arrange, first))


def assemble(step, fetched, green):
    own_ref, side_ref, cross_ref, down_ref = fetched
    half = own_ref.shape[-1]

    def fill(mine):
        for blocks, row, column in (
            (own_ref, 0, mine),
            (side_ref, 0, 1 - mine),
            (cross_ref, 1, 1 - mine),
            (down_ref, 1, mine),
        ):
            for part in range(2):
                start = (2 * row + part) * half
                green[column, start : start + half, :] = blocks[step, part]

    for mine in range(2):
        pl.when(lax.rem(row_bit() + core_bit(), 2) == mine)(functools.partial(fill, mine))


def step_products(source, target, green, products, surface_from, surface):
    order = source[0].shape[0] // 2
    half = order // 2
    for coupling, product in zip(source, products):
        for h in range(2):
            place(product, h, dot(coupling[...], green[h]).astype(jnp.bfloat16))
    for h in range(2):
        term = dot(products[0][:order, :], column_of(source[1], h))
        columns = slice(h * half, (h + 1) * half)
        surface[:, columns] = term if surface_from is None else surface_from[:, columns] + term
    for product, coupling, following in zip(products, source, target):
        for h in range(2):
            place(following, h, dot(product[...], column_of(coupling, h)).astype(jnp.bfloat16))


def first_steps(
    forward_in, backward_in, own_ref, side_ref, cross_ref, down_ref,
    forward, backward, surface, green, forward_green, backward_green,
):
    source, target = (forward_in, backward_in), (forward, backward)
    surface_from = None
    for step in range(CHUNK):
        assemble(step, (own_ref, side_ref, cross_ref, down_ref), green)
        step_products(source, target, green, (forward_green, backward_green), surface_from, surface)
        source, surface_from = target, surface


def last_steps(
    forward_in, backward_in, surface_in, drive_ref, own_ref, side_ref, cross_ref, down_ref,
    forward_out, backward_out, green_out, forward_rows_out, injected,
    forward, backward, green, forward_rows, surface, forward_green, backward_green, copy_sems,
):
    fetched = (own_ref, side_ref, cross_ref, down_ref)
    leaving = (forward, backward, green, forward_rows)
    outs = (forward_out, backward_out, green_out, forward_rows_out)
    copies = [
        pltpu.make_async_copy(kept, out, copy_sems.at[i])
        for i, (kept, out) in enumerate(zip(leaving, outs))
    ]
    source, target = (forward_in, backward_in), (forward, backward)
    surface_from = surface_in
    for step in range(CHUNK - 1):
        assemble(step, fetched, green)
        step_products(source, target, green, (forward_green, backward_green), surface_from, surface)
        source, surface_from = target, surface
    copies[0].start()
    copies[1].start()
    assemble(CHUNK - 1, fetched, green)
    copies[2].start()
    order = forward.shape[0] // 2
    half = order // 2
    for h in range(2):
        place(forward_rows, h, dot(forward[:order, :], green[h]).astype(jnp.bfloat16))
    copies[3].start()
    energy = []
    for h in range(2):
        term = dot(forward_rows[...], column_of(backward, h))
        energy.append((surface[:, h * half : (h + 1) * half] + term).astype(jnp.bfloat16))
    value = lax.dot_general(
        drive_ref[...],
        jnp.concatenate([e[part * half : (part + 1) * half] for part in range(2) for e in energy], axis=1),
        (((1,), (1,)), ((), ())),
        preferred_element_type=jnp.float32,
    ).astype(jnp.bfloat16)
    block_rows, _, count, _ = injected.shape
    rows = block_rows * count
    for part in range(2):
        injected[:, part] = value[part * rows : (part + 1) * rows].reshape(block_rows, count, half)
    for copy in copies:
        copy.wait()


def far_blocks(
    forward_in, backward_in, green_in, forward_rows_in, kept_ref, given_ref,
    forward, backward, green, forward_rows, backward_rows, copy_sems,
):
    arriving = (backward_in, green_in, forward_rows_in, forward_in)
    held = (backward, green, forward_rows, forward)
    copies = [
        pltpu.make_async_copy(source, kept, copy_sems.at[i])
        for i, (source, kept) in enumerate(zip(arriving, held))
    ]
    for copy in copies:
        copy.start()
    order = forward.shape[0] // 2
    half = order // 2
    mine = lax.rem(row_bit() + core_bit(), 2)
    copies[0].wait()
    copies[1].wait()
    for h in range(2):
        place(backward_rows, h, dot(backward[:order, :], green[h]).astype(jnp.bfloat16))
    copies[2].wait()
    copies[3].wait()
    for which, rows, coupling in ((0, forward_rows, forward), (1, backward_rows, backward)):
        for h in range(2):
            value = dot(rows[...], column_of(coupling, h)).astype(jnp.bfloat16)

            @pl.when(mine == h)
            def _():
                kept_ref[which, 0] = value[:half]
                kept_ref[which, 1] = value[half:]

            @pl.when(mine != h)
            def _():
                given_ref[which, 0] = value[:half]
                given_ref[which, 1] = value[half:]


def choose(kept_ref, given_ref, forward_ref, backward_ref):
    worker = lax.rem(lax.axis_index("rows"), 2) == core_bit()
    for which, far_ref in enumerate((forward_ref, backward_ref)):
        far_ref[0] = jnp.where(worker, kept_ref[which], given_ref[which])


def spread(assignment_ref, weight_ref, received_ref, injection_ref, weighted_ref):
    groups = injection_ref.shape[0]
    half = received_ref.shape[-1]
    column = core_bit()
    for part in range(2):
        for a in range(2):
            total = jnp.zeros(injection_ref.shape[2:3] + (half,), jnp.float32)
            for slot in range(groups):
                e = lax.rem(assignment_ref[slot], groups)
                value = received_ref[slot, a, column, part].astype(jnp.float32)
                injection_ref[e, part, :, a * half : (a + 1) * half] = value
                total = total + weight_ref[e] * value
            weighted_ref[part, :, a * half : (a + 1) * half] = total.astype(weighted_ref.dtype)


def in_hbm(*arrays):
    return [pltpu.with_memory_space_constraint(array, pltpu.HBM) for array in arrays]


def call(body, outs, scratch, scalars=0, vmem=32, far_outs=0, far_ins=0):
    def run(*operands):
        specs = [SMEM_WHOLE] * scalars + [VMEM_WHOLE] * (len(operands) - scalars)
        specs[:far_ins] = [HBM_WHOLE] * far_ins
        return pl.pallas_call(
            body,
            out_shape=outs,
            in_specs=specs,
            out_specs=tuple(HBM_WHOLE if i < far_outs else VMEM_WHOLE for i in range(len(outs))),
            scratch_shapes=scratch,
            compiler_params=pltpu.CompilerParams(vmem_limit_bytes=vmem * MIB),
        )(*operands)

    return run


def over_energies(energies_axis, own):
    chips = energies_axis // 2
    assert chips == 8

    def from_chip(value, distance):
        pairs = [
            ((chip + distance) % chips * 2 + core, chip * 2 + core)
            for chip in range(chips)
            for core in range(2)
        ]
        return lax.ppermute(value, "energy", pairs)

    after = from_chip(own, 1)
    before = from_chip(own, -1)
    two = own.astype(jnp.float32) + after.astype(jnp.float32)
    three = two + before.astype(jnp.float32)
    ahead = from_chip(three.astype(own.dtype), 3)
    behind = from_chip(two.astype(own.dtype), -3)
    return three + ahead.astype(jnp.float32) + behind.astype(jnp.float32)


def local(energies_axis, rows_axis, coupling, inverses, contact_row, assignment, states, weights):
    half = inverses.shape[-1]
    order = 2 * half
    slots = rows_axis // 4
    bf16, f32 = jnp.bfloat16, jnp.float32
    both = ("energy", "rows")

    def routes(flip, to_worker):
        pairs = []
        for energy in range(energies_axis):
            for slot in range(slots):
                for x in range(4):
                    if (x % 2 == energy % 2) == to_worker:
                        base = energy * rows_axis + slot * 4
                        pairs.append((base + (x ^ flip), base + x))
        return pairs

    chunks = [inverses[0, CHUNK * c : CHUNK * (c + 1)] for c in range(ITERS // CHUNK)]
    fetched = []
    for c, chunk in enumerate(chunks):
        fetched.append([])
        for flip in FLIPS:
            fetched[c].append(lax.ppermute(chunk, both, routes(flip, True)))

    square = jax.ShapeDtypeStruct((2 * order, 2 * order), bf16)
    count = states.shape[2]
    block_rows = rows_axis
    forward, backward, drive = call(
        prepare,
        (square, square, jax.ShapeDtypeStruct((2 * block_rows * count, 2 * order), bf16)),
        [pltpu.VMEM((block_rows, 2, count, order), f32)],
        scalars=1,
    )(contact_row, coupling, states)

    square_scratch = pltpu.VMEM((2 * order, 2 * order), bf16)
    green_shape = (2, 2 * order, half)
    surface_shape = (order, order)
    rows_scratch = pltpu.VMEM((order, 2 * order), bf16)
    forward, backward, surface = call(
        first_steps,
        (square, square, jax.ShapeDtypeStruct(surface_shape, f32)),
        [pltpu.VMEM(green_shape, bf16), square_scratch, square_scratch],
    )(forward, backward, chunks[0], *fetched[0])
    forward, backward, green, forward_rows, injected = call(
        last_steps,
        (
            pltpu.HBM((2 * order, 2 * order), bf16),
            pltpu.HBM((2 * order, 2 * order), bf16),
            pltpu.HBM(green_shape, bf16),
            pltpu.HBM((order, 2 * order), bf16),
            jax.ShapeDtypeStruct((block_rows, 2, count, half), bf16),
        ),
        [
            square_scratch,
            square_scratch,
            pltpu.VMEM(green_shape, bf16),
            rows_scratch,
            pltpu.VMEM(surface_shape, f32),
            square_scratch,
            square_scratch,
            pltpu.SemaphoreType.DMA((4,)),
        ],
        far_outs=4,
    )(forward, backward, surface, drive, chunks[1], *fetched[1])

    received = lax.all_to_all(injected, "rows", split_axis=0, concat_axis=0, tiled=True)

    far_shape = jax.ShapeDtypeStruct((2, 2, half, half), bf16)
    kept, given = call(
        far_blocks,
        (far_shape, far_shape),
        [
            square_scratch,
            square_scratch,
            pltpu.VMEM(green_shape, bf16),
            rows_scratch,
            rows_scratch,
            pltpu.SemaphoreType.DMA((4,)),
        ],
        far_ins=4,
    )(*in_hbm(forward, backward, green, forward_rows))
    given = lax.ppermute(given, both, routes(1, False))
    block_shape = jax.ShapeDtypeStruct((1, 2, half, half), bf16)
    far_forward, far_backward = call(choose, (block_shape, block_shape), [])(kept, given)

    groups = assignment.shape[0]
    injection, weighted = call(
        spread,
        (
            jax.ShapeDtypeStruct((groups, 2, count, order), f32),
            jax.ShapeDtypeStruct((2, count, order), bf16),
        ),
        [],
        scalars=2,
    )(assignment, weights, received.reshape(slots, 2, 2, 2, count, half))
    total = over_energies(energies_axis, weighted)
    other = lax.ppermute(total.astype(bf16), "energy", [(i, i ^ 1) for i in range(energies_axis)])
    integrated = total + other.astype(f32)
    return injection[:, None], integrated[None], far_forward, far_backward


def solution(mesh):
    def whole(*operands):
        return local(mesh.shape["energy"], mesh.shape["rows"], *operands)

    placed = (
        P(),
        P(("energy", "rows"), None, None, None, None),
        P(),
        P("energy"),
        P(),
        P("energy"),
    )
    return jax.shard_map(
        whole,
        mesh=mesh,
        in_specs=placed,
        out_specs=(
            P("energy", "rows", None, None, None),
            P("rows", None, None, None),
            P(("energy", "rows"), None, None, None),
            P(("energy", "rows"), None, None, None),
        ),
        check_vma=False,
    )
```

```python
import functools

import jax
import jax.numpy as jnp
from jax import lax
from jax.experimental import pallas as pl
from jax.experimental.pallas import tpu as pltpu
from jax.sharding import PartitionSpec as P


ITERS = 4
CHUNK = 2
FLIPS = (1, 3, 2)
VMEM_WHOLE = pl.BlockSpec(memory_space=pltpu.VMEM)
SMEM_WHOLE = pl.BlockSpec(memory_space=pltpu.SMEM)
HBM_WHOLE = pl.BlockSpec(memory_space=pltpu.HBM)
MIB = 1 << 20


def dot(left, right):
    return jnp.dot(left, right, preferred_element_type=jnp.float32)


def row_bit():
    return lax.rem(lax.div(lax.axis_index("rows"), 2), 2)


def core_bit():
    return lax.rem(lax.axis_index("energy"), 2)


def place(ref, column_half, value):
    half = value.shape[1]
    start = column_half * 2 * half
    ref[:, start : start + half] = value
    for row in range(0, value.shape[0], 2 * half):
        ref[row : row + half, start + half : start + 2 * half] = -value[row + half : row + 2 * half]
        ref[row + half : row + 2 * half, start + half : start + 2 * half] = value[row : row + half]


def column_of(matrix, column_half):
    half = matrix.shape[1] // 4
    return matrix[:, column_half * 2 * half : column_half * 2 * half + half]


def prepare(row_ref, coupling_ref, states_ref, forward_ref, backward_ref, drive_ref, sums):
    order = coupling_ref.shape[-1]
    half = order // 2
    sums[...] = jnp.zeros_like(sums)

    @pl.loop(0, states_ref.shape[0])
    def _(contact):
        row = row_ref[contact]
        sums[row] = sums[row] + states_ref[contact].astype(jnp.float32)

    block_rows, _, count, _ = sums.shape
    count = block_rows * count

    def arrange(first):
        def block(part, i, j):
            rows, columns = ((first ^ k) * half for k in (i, j))
            return coupling_ref[part, rows : rows + half, columns : columns + half]

        for j in range(2):
            ahead, back = [], []
            for i in range(2):
                ahead += [block(0, i, j), block(1, i, j)]
                back += [block(0, j, i).T, -block(1, j, i).T]
            place(forward_ref, j, jnp.concatenate(ahead, axis=0))
            place(backward_ref, j, jnp.concatenate(back, axis=0))
        for h in range(2):
            left = h * half
            right = order + left
            start = (first ^ h) * half
            real, imag = (
                sums[:, part, :, start : start + half].astype(jnp.bfloat16).reshape(count, half)
                for part in range(2)
            )
            drive_ref[:count, left : left + half] = real
            drive_ref[count:, left : left + half] = imag
            drive_ref[:count, right : right + half] = -imag
            drive_ref[count:, right : right + half] = real

    for first in range(2):
        pl.when(row_bit() == first)(functools.partial(arrange, first))


def assemble(step, fetched, green):
    own_ref, side_ref, cross_ref, down_ref = fetched
    half = own_ref.shape[-1]

    def fill(mine):
        for blocks, row, column in (
            (own_ref, 0, mine),
            (side_ref, 0, 1 - mine),
            (cross_ref, 1, 1 - mine),
            (down_ref, 1, mine),
        ):
            for part in range(2):
                start = (2 * row + part) * half
                green[column, start : start + half, :] = blocks[step, part]

    for mine in range(2):
        pl.when(lax.rem(row_bit() + core_bit(), 2) == mine)(functools.partial(fill, mine))


def step_products(source, target, green, products, surface_from, surface):
    order = source[0].shape[0] // 2
    half = order // 2
    for coupling, product in zip(source, products):
        for h in range(2):
            place(product, h, dot(coupling[...], green[h]).astype(jnp.bfloat16))
    for h in range(2):
        term = dot(products[0][:order, :], column_of(source[1], h))
        columns = slice(h * half, (h + 1) * half)
        surface[:, columns] = term if surface_from is None else surface_from[:, columns] + term
    for product, coupling, following in zip(products, source, target):
        for h in range(2):
            place(following, h, dot(product[...], column_of(coupling, h)).astype(jnp.bfloat16))


def first_steps(
    forward_in, backward_in, own_ref, side_ref, cross_ref, down_ref,
    forward, backward, surface, green, forward_green, backward_green,
):
    source, target = (forward_in, backward_in), (forward, backward)
    surface_from = None
    for step in range(CHUNK):
        assemble(step, (own_ref, side_ref, cross_ref, down_ref), green)
        step_products(source, target, green, (forward_green, backward_green), surface_from, surface)
        source, surface_from = target, surface


def last_steps(
    forward_in, backward_in, surface_in, drive_ref, own_ref, side_ref, cross_ref, down_ref,
    forward_out, backward_out, green_out, forward_rows_out, injected,
    forward, backward, green, forward_rows, surface, forward_green, backward_green, copy_sems,
):
    fetched = (own_ref, side_ref, cross_ref, down_ref)
    leaving = (forward, backward, green, forward_rows)
    outs = (forward_out, backward_out, green_out, forward_rows_out)
    copies = [
        pltpu.make_async_copy(kept, out, copy_sems.at[i])
        for i, (kept, out) in enumerate(zip(leaving, outs))
    ]
    source, target = (forward_in, backward_in), (forward, backward)
    surface_from = surface_in
    for step in range(CHUNK - 1):
        assemble(step, fetched, green)
        step_products(source, target, green, (forward_green, backward_green), surface_from, surface)
        source, surface_from = target, surface
    copies[0].start()
    copies[1].start()
    assemble(CHUNK - 1, fetched, green)
    copies[2].start()
    order = forward.shape[0] // 2
    half = order // 2
    for h in range(2):
        place(forward_rows, h, dot(forward[:order, :], green[h]).astype(jnp.bfloat16))
    copies[3].start()
    energy = []
    for h in range(2):
        term = dot(forward_rows[...], column_of(backward, h))
        energy.append((surface[:, h * half : (h + 1) * half] + term).astype(jnp.bfloat16))
    value = lax.dot_general(
        drive_ref[...],
        jnp.concatenate([e[part * half : (part + 1) * half] for part in range(2) for e in energy], axis=1),
        (((1,), (1,)), ((), ())),
        preferred_element_type=jnp.float32,
    ).astype(jnp.bfloat16)
    block_rows, _, count, _ = injected.shape
    rows = block_rows * count
    for part in range(2):
        injected[:, part] = value[part * rows : (part + 1) * rows].reshape(block_rows, count, half)
    for copy in copies:
        copy.wait()


def far_blocks(
    forward_in, backward_in, green_in, forward_rows_in, kept_ref, given_ref,
    forward, backward, green, forward_rows, backward_rows, copy_sems,
):
    arriving = (backward_in, green_in, forward_rows_in, forward_in)
    held = (backward, green, forward_rows, forward)
    copies = [
        pltpu.make_async_copy(source, kept, copy_sems.at[i])
        for i, (source, kept) in enumerate(zip(arriving, held))
    ]
    for copy in copies:
        copy.start()
    order = forward.shape[0] // 2
    half = order // 2
    mine = lax.rem(row_bit() + core_bit(), 2)
    copies[0].wait()
    copies[1].wait()
    for h in range(2):
        place(backward_rows, h, dot(backward[:order, :], green[h]).astype(jnp.bfloat16))
    copies[2].wait()
    copies[3].wait()
    for which, rows, coupling in ((0, forward_rows, forward), (1, backward_rows, backward)):
        for h in range(2):
            value = dot(rows[...], column_of(coupling, h)).astype(jnp.bfloat16)

            @pl.when(mine == h)
            def _():
                kept_ref[which, 0] = value[:half]
                kept_ref[which, 1] = value[half:]

            @pl.when(mine != h)
            def _():
                given_ref[which, 0] = value[:half]
                given_ref[which, 1] = value[half:]


def choose(kept_ref, given_ref, forward_ref, backward_ref):
    worker = lax.rem(lax.axis_index("rows"), 2) == core_bit()
    for which, far_ref in enumerate((forward_ref, backward_ref)):
        far_ref[0] = jnp.where(worker, kept_ref[which], given_ref[which])


def spread(assignment_ref, weight_ref, received_ref, injection_ref, weighted_ref):
    groups = injection_ref.shape[0]
    half = received_ref.shape[-1]
    column = core_bit()
    for part in range(2):
        for a in range(2):
            total = jnp.zeros(injection_ref.shape[2:3] + (half,), jnp.float32)
            for slot in range(groups):
                e = lax.rem(assignment_ref[slot], groups)
                value = received_ref[slot, a, column, part].astype(jnp.float32)
                injection_ref[e, part, :, a * half : (a + 1) * half] = value
                total = total + weight_ref[e] * value
            total = total.astype(weighted_ref.dtype)
            for copy in range(weighted_ref.shape[0]):
                weighted_ref[copy, part, :, a * half : (a + 1) * half] = total


def in_hbm(*arrays):
    return [pltpu.with_memory_space_constraint(array, pltpu.HBM) for array in arrays]


def call(body, outs, scratch, scalars=0, vmem=32, far_outs=0, far_ins=0):
    def run(*operands):
        specs = [SMEM_WHOLE] * scalars + [VMEM_WHOLE] * (len(operands) - scalars)
        specs[:far_ins] = [HBM_WHOLE] * far_ins
        return pl.pallas_call(
            body,
            out_shape=outs,
            in_specs=specs,
            out_specs=tuple(HBM_WHOLE if i < far_outs else VMEM_WHOLE for i in range(len(outs))),
            scratch_shapes=scratch,
            compiler_params=pltpu.CompilerParams(vmem_limit_bytes=vmem * MIB),
        )(*operands)

    return run


def over_energies(energies_axis, copies):
    chips = energies_axis // 2
    alike = [[2 * chip + core for chip in range(chips)] for core in range(2)]
    couples = [[2 * chip, 2 * chip + 1] for chip in range(chips)]
    gathered = lax.all_to_all(
        copies, "energy", split_axis=0, concat_axis=0, axis_index_groups=alike, tiled=True
    )
    own = jnp.sum(gathered.astype(jnp.float32), axis=0).astype(copies.dtype)
    both = lax.all_to_all(
        jnp.stack([own, own]),
        "energy",
        split_axis=0,
        concat_axis=0,
        axis_index_groups=couples,
        tiled=True,
    )
    return jnp.sum(both.astype(jnp.float32), axis=0)


def local(energies_axis, rows_axis, coupling, inverses, contact_row, assignment, states, weights):
    half = inverses.shape[-1]
    order = 2 * half
    slots = rows_axis // 4
    bf16, f32 = jnp.bfloat16, jnp.float32
    both = ("energy", "rows")

    def routes(flip, to_worker):
        pairs = []
        for energy in range(energies_axis):
            for slot in range(slots):
                for x in range(4):
                    if (x % 2 == energy % 2) == to_worker:
                        base = energy * rows_axis + slot * 4
                        pairs.append((base + (x ^ flip), base + x))
        return pairs

    chunks = [inverses[0, CHUNK * c : CHUNK * (c + 1)] for c in range(ITERS // CHUNK)]
    fetched = []
    for c, chunk in enumerate(chunks):
        fetched.append([])
        for flip in FLIPS:
            fetched[c].append(lax.ppermute(chunk, both, routes(flip, True)))

    square = jax.ShapeDtypeStruct((2 * order, 2 * order), bf16)
    count = states.shape[2]
    block_rows = rows_axis
    forward, backward, drive = call(
        prepare,
        (square, square, jax.ShapeDtypeStruct((2 * block_rows * count, 2 * order), bf16)),
        [pltpu.VMEM((block_rows, 2, count, order), f32)],
        scalars=1,
    )(contact_row, coupling, states)

    square_scratch = pltpu.VMEM((2 * order, 2 * order), bf16)
    green_shape = (2, 2 * order, half)
    surface_shape = (order, order)
    rows_scratch = pltpu.VMEM((order, 2 * order), bf16)
    forward, backward, surface = call(
        first_steps,
        (square, square, jax.ShapeDtypeStruct(surface_shape, f32)),
        [pltpu.VMEM(green_shape, bf16), square_scratch, square_scratch],
    )(forward, backward, chunks[0], *fetched[0])
    forward, backward, green, forward_rows, injected = call(
        last_steps,
        (
            pltpu.HBM((2 * order, 2 * order), bf16),
            pltpu.HBM((2 * order, 2 * order), bf16),
            pltpu.HBM(green_shape, bf16),
            pltpu.HBM((order, 2 * order), bf16),
            jax.ShapeDtypeStruct((block_rows, 2, count, half), bf16),
        ),
        [
            square_scratch,
            square_scratch,
            pltpu.VMEM(green_shape, bf16),
            rows_scratch,
            pltpu.VMEM(surface_shape, f32),
            square_scratch,
            square_scratch,
            pltpu.SemaphoreType.DMA((4,)),
        ],
        far_outs=4,
    )(forward, backward, surface, drive, chunks[1], *fetched[1])

    received = lax.all_to_all(injected, "rows", split_axis=0, concat_axis=0, tiled=True)

    far_shape = jax.ShapeDtypeStruct((2, 2, half, half), bf16)
    kept, given = call(
        far_blocks,
        (far_shape, far_shape),
        [
            square_scratch,
            square_scratch,
            pltpu.VMEM(green_shape, bf16),
            rows_scratch,
            rows_scratch,
            pltpu.SemaphoreType.DMA((4,)),
        ],
        far_ins=4,
    )(*in_hbm(forward, backward, green, forward_rows))
    given = lax.ppermute(given, both, routes(1, False))
    block_shape = jax.ShapeDtypeStruct((1, 2, half, half), bf16)
    far_forward, far_backward = call(choose, (block_shape, block_shape), [])(kept, given)

    groups = assignment.shape[0]
    injection, weighted = call(
        spread,
        (
            jax.ShapeDtypeStruct((groups, 2, count, order), f32),
            jax.ShapeDtypeStruct((energies_axis // 2, 2, count, order), bf16),
        ),
        [],
        scalars=2,
    )(assignment, weights, received.reshape(slots, 2, 2, 2, count, half))
    integrated = over_energies(energies_axis, weighted)
    return injection[:, None], integrated[None], far_forward, far_backward


def solution(mesh):
    def whole(*operands):
        return local(mesh.shape["energy"], mesh.shape["rows"], *operands)

    placed = (
        P(),
        P(("energy", "rows"), None, None, None, None),
        P(),
        P("energy"),
        P(),
        P("energy"),
    )
    return jax.shard_map(
        whole,
        mesh=mesh,
        in_specs=placed,
        out_specs=(
            P("energy", "rows", None, None, None),
            P("rows", None, None, None),
            P(("energy", "rows"), None, None, None),
            P(("energy", "rows"), None, None, None),
        ),
        check_vma=False,
    )
```
